128 devices in a mesh: prow: 8 (over y, x_lo), pcol: 16 (over x_hi, z, core).
Axes of the slice: x: 4 (x_hi: 2, x_lo: 2; x = x_hi * 2 + x_lo), y: 4, z: 4, core: 2. Of those that a mesh axis runs over, the one named last changes fastest.
Arguments:
- covariance: float32 [16384, 16384], P(('prow', 'pcol')), may hold values from -600 to 600, as said below
- factor_left: float32 [64, 16384], P(None, ('prow', 'pcol')), may hold values from -6 to 6
- factor_right: float32 [64, 16384], P('prow', 'pcol'), may hold values from -3 to 3
Outputs:
- whitened: float32 [16384, 16384], P('prow', 'pcol')
The draws below stay inside these ranges and needn't reach their ends.
Inputs may be any that keep to these rules, and one draw needn't show every extreme that they name: `covariance`: entries are real-valued and of full rank.
All inputs are finite; a program needn't handle non-finite values.
Results may differ from the reference program's by a relative error of at most 0.00007.
Values sent between devices are 32-bit elements; how exact they have to be, the bound alone decides.
No kernel may reach another device: no remote copies, remote signals or barrier semaphores. Data moves between devices by JAX's collectives and lax.ppermute only.
A program may use at most 128 MiB of HBM per device.

```python
import jax
import jax.numpy as jnp
from jax import lax

ORDER = 16384
RANK = 64
TILE = 64
N_PROW = 8
N_PCOL = 16


def draw_covariance(key, part):
    subkeys = jax.random.split(key, 3)
    positions = jnp.arange(ORDER)
    tile_row = (positions // TILE % N_PROW).astype(jnp.float32)
    tile_col = (positions // TILE % N_PCOL).astype(jnp.float32)
    row_scale = jnp.exp(tile_row / (N_PROW - 1) * jnp.log(3.0) + jax.random.uniform(subkeys[0], (ORDER,)) * jnp.log(3.3))
    col_scale = jnp.exp(tile_col / (N_PCOL - 1) * jnp.log(3.0) + jax.random.uniform(subkeys[1], (ORDER,)) * jnp.log(3.3))
    noise = jnp.clip(jax.random.normal(subkeys[2], (ORDER, ORDER), jnp.float32), -6.0, 6.0)
    return (noise * row_scale[:, None] * col_scale[None, :]).astype(jnp.float32)


def level_of(key, dims, cuts, smallest, high):
    def one(dim, parts):
        heights = jax.random.uniform(jax.random.fold_in(jax.random.fold_in(key, 6), dim), (parts,), jnp.float32, smallest / len(cuts), high / len(cuts))
        return jnp.repeat(jnp.exp(heights), dims[dim] // parts).reshape((-1,) + (1,) * (len(dims) - dim - 1))

    level = one(*cuts[0])
    for cut in cuts[1:]:
        level = level * one(*cut)
    return level


def centred(stream_key, extent, spread, reach, cuts=(), dtype=jnp.bfloat16):
    loudness = level_of(stream_key, extent, cuts, -0.22, 0.18) if cuts else 1.0
    result = jax.random.normal(stream_key, extent, jnp.float32) * spread * loudness
    return jnp.minimum(jnp.maximum(result, -reach), reach).astype(dtype)


def setup_inputs(seed: int = 0) -> dict:
    key_of = jax.random.split(jax.random.key(seed), 4)
    return {
        "covariance": draw_covariance(jax.random.fold_in(key_of[3], 71), 0),
        "factor_left": centred(key_of[1], (RANK, ORDER), 1.0, 6.0, ((1, 128),), jnp.float32),
        "factor_right": centred(key_of[2], (RANK, ORDER), 0.5, 3.0, ((0, 8), (1, 16)), jnp.float32),
    }


epsilon = 1e-06

def reference(covariance, factor_left, factor_right):
    grid_rows = N_PROW
    grid_cols = N_PCOL
    tiles_down = ORDER // (TILE * grid_rows)
    tiles_across = ORDER // (TILE * grid_cols)
    natural = factor_right.reshape(RANK, grid_cols, tiles_across, TILE).transpose(0, 2, 1, 3).reshape(RANK, ORDER)
    corrected = covariance + jnp.dot(factor_left.T, natural, precision=lax.Precision.HIGHEST, preferred_element_type=jnp.float32)
    squared = corrected * corrected
    row_mean = lax.optimization_barrier(jnp.sum(squared, axis=1)) / ORDER + epsilon
    col_mean = lax.optimization_barrier(jnp.sum(squared, axis=0)) / ORDER + epsilon
    scaled = corrected * lax.rsqrt(jnp.sqrt(row_mean[:, None] * col_mean[None, :]))
    placed = scaled.reshape(tiles_down, grid_rows, TILE, tiles_across, grid_cols, TILE)
    return placed.transpose(1, 0, 2, 4, 3, 5).reshape(ORDER, ORDER)
```

```python
import functools

import jax
import jax.numpy as jnp
from jax import lax
from jax.experimental import pallas as pl
from jax.experimental.pallas import tpu as pltpu
from jax.sharding import Mesh
from jax.sharding import PartitionSpec as P


ORDER = 16384
TILE = 64
epsilon = 1e-06
F32 = jnp.float32

NAMES = ("y", "xl", "xh", "z1", "z0", "c")
ROWS = ("y", "xl")
COLS = ("xh", "z1", "z0", "c")
ZC = ("z1", "z0", "c")
SPREAD = ("y", "xl", "xh", "z1")

CHUNKS = (1, 3)


def flip(pairing, dz, dc):
    pairs = []
    for z1 in range(2):
        for z0 in range(2):
            for c in range(2):
                to = z1 ^ (dz if pairing == 2 else 0), z0 ^ dz, c ^ dc
                pairs.append((z1 * 4 + z0 * 2 + c, to[0] * 4 + to[1] * 2 + to[2]))
    return pairs


def pack_kernel(with_left, x_ref, *refs):
    if with_left:
        left_ref, refs = refs[0], refs[1:]
    z0 = lax.axis_index("z0")
    odd = lax.axis_index("c") == 1
    r = pl.program_id(0)
    low = lax.broadcasted_iota(jnp.int32, (TILE, 128), 1) < TILE
    for dz in range(2):
        for xh in range(2):
            for z1 in range(2):
                at = pl.multiple_of((xh * 4 + z1 * 2 + (z0 ^ dz)) * 128, 128)
                a = x_ref[:, pl.ds(at, 128)]
                b = x_ref[:, pl.ds(at + 1024, 128)]
                even_tiles = jnp.where(low, a, pltpu.roll(b, 64, 1))
                odd_tiles = jnp.where(low, pltpu.roll(a, 64, 1), b)
                slot = xh * 2 + z1
                refs[dz * 2][slot, 0:TILE, :] = jnp.where(odd, odd_tiles, even_tiles)
                refs[dz * 2 + 1][slot, 0:TILE, :] = jnp.where(odd, even_tiles, odd_tiles)
    if with_left:
        both = left_ref[...]
        shifted = pltpu.roll(both, 64, 1)
        top = jnp.where(r == 0, both, shifted)
        bottom = jnp.where(r == 0, shifted, both)
        packed = jnp.where(low[0:32], top[0:32], bottom[32:64])
        for ref in refs:
            for slot in range(4):
                ref[slot, TILE : TILE + 32, :] = packed


def pack(x, left, start, count):
    with_left = left is not None
    height = TILE + 32 if with_left else TILE
    assert count == 1 or not with_left
    in_specs = [pl.BlockSpec((TILE, 2048), lambda r, j: (r, start + j))]
    args = [x]
    if with_left:
        in_specs.append(pl.BlockSpec((64, 128), lambda r, j: (0, 0)))
        args.append(left)
    return pl.pallas_call(
        functools.partial(pack_kernel, with_left),
        grid=(2, count),
        in_specs=in_specs,
        out_specs=[pl.BlockSpec((4, height, 128), lambda r, j: (r, j, 0))] * 4,
        out_shape=[jax.ShapeDtypeStruct((8, height * count, 128), F32)] * 4,
        name="pack",
    )(*args)


def assemble_kernel(heights, *refs):
    pieces, out_ref = refs[:-1], refs[-1]
    own = lax.axis_index("z0") * 2 + lax.axis_index("c")
    at = 0
    for g, height in enumerate(heights):
        for d in range(4):
            out_ref[own ^ d, :, at : at + height, :] = pieces[g * 4 + d][...]
        at += height


def assemble(groups):
    heights = tuple(g[0].shape[1] for g in groups)
    total = sum(heights)
    whole = pl.pallas_call(
        functools.partial(assemble_kernel, heights),
        grid=(8,),
        in_specs=[pl.BlockSpec((1, h, 128), lambda i: (i, 0, 0)) for h in heights for _ in range(4)],
        out_specs=pl.BlockSpec((4, 1, total, 128), lambda i: (0, i, 0, 0)),
        out_shape=jax.ShapeDtypeStruct((4, 8, total, 128), F32),
        name="assemble",
    )(*[p for g in groups for p in g])
    return whole.reshape(32, total, 128)


def correct_kernel(offsets, swapped, got_ref, left_ref, right_ref, out_ref, row_ref, col_ref):
    step = pl.program_id(0)
    product = jnp.dot(left_ref[...], right_ref[...], preferred_element_type=F32)
    turn = (lax.axis_index("y") // 2) ^ lax.axis_index("z0")
    row_acc = jnp.zeros((256, 128), F32)

    @pl.when(step == 0)
    def _():
        col_ref[...] = jnp.zeros_like(col_ref)

    for j, (at, swap) in enumerate(zip(offsets, swapped)):
        cols = slice(j * 128, j * 128 + 128)
        parts = []
        for k in range(4):
            source = (k ^ turn) if swap else k
            parts.append(got_ref[source, at : at + TILE, :] + product[k * TILE : k * TILE + TILE, cols])
        tile = jnp.concatenate(parts, 0)
        out_ref[:, cols] = tile
        square = tile * tile
        row_acc = row_acc + square
        col_ref[:, cols] += jnp.sum(square.reshape(32, 8, 128), 0)
    row_ref[0] = lax.dot_general(
        jnp.ones((8, 128), F32),
        row_acc,
        (((1,), (1,)), ((), ())),
        precision=lax.Precision.HIGHEST,
        preferred_element_type=F32,
    )


def correct(got, left, right, start, offsets, swapped):
    width = 128 * len(offsets)
    assert (start * 128) % width == 0
    return pl.pallas_call(
        functools.partial(correct_kernel, offsets, swapped),
        grid=(8,),
        in_specs=[
            pl.BlockSpec((4, got.shape[1], 128), lambda i: (i, 0, 0)),
            pl.BlockSpec((256, 256), lambda i: (i, 0)),
            pl.BlockSpec((256, width), lambda i: (0, 0)),
        ],
        out_specs=[
            pl.BlockSpec((256, width), lambda i: (i, 0)),
            pl.BlockSpec((1, 8, 256), lambda i: (i, 0, 0)),
            pl.BlockSpec((8, width), lambda i: (0, 0)),
        ],
        out_shape=[
            jax.ShapeDtypeStruct((2048, width), F32),
            jax.ShapeDtypeStruct((8, 8, 256), F32),
            jax.ShapeDtypeStruct((8, width), F32),
        ],
        name="correct",
    )(got, left, right)


def scale_kernel(widths, *refs):
    n = len(widths)
    row_ref, col_ref, out_ref = refs[n:]
    row = jnp.transpose(jnp.broadcast_to(row_ref[0], (128, 256)))
    at = 0
    for ref, width in zip(refs, widths):
        for j in range(width // 128):
            cols = slice(at, at + 128)
            out_ref[:, cols] = ref[:, j * 128 : j * 128 + 128] * (row * col_ref[:, cols])
            at += 128


def scale(parts, row, col):
    widths = tuple(p.shape[1] for p in parts)
    return pl.pallas_call(
        functools.partial(scale_kernel, widths),
        grid=(8,),
        in_specs=[pl.BlockSpec((256, w), lambda i: (i, 0)) for w in widths]
        + [pl.BlockSpec((1, 1, 256), lambda i: (i, 0, 0)), pl.BlockSpec((1, 1024), lambda i: (0, 0))],
        out_specs=pl.BlockSpec((256, 1024), lambda i: (i, 0)),
        out_shape=jax.ShapeDtypeStruct((2048, 1024), F32),
        name="scale",
    )(*parts, row.reshape(8, 1, 256), col.reshape(1, 1024))


def split(x):
    high = lax.reduce_precision(x, 8, 7)
    low = lax.reduce_precision(x - high, 8, 7)
    return high.astype(jnp.bfloat16), low.astype(jnp.bfloat16)


ROUNDS = (
    ("xl", [(0, 1), (1, 0)], lambda: lax.axis_index("xl")),
    ("y", [(0, 1), (1, 0), (2, 3), (3, 2)], lambda: lax.axis_index("y") % 2),
    ("y", [(0, 2), (2, 0), (1, 3), (3, 1)], lambda: lax.axis_index("y") // 2),
)


def gather_right(part):
    for axis, pairs, bit in ROUNDS:
        other = lax.ppermute(part, axis, pairs)
        first = bit() == 0
        part = jnp.where(first, jnp.concatenate([part, other]), jnp.concatenate([other, part]))
    return part


def sum_over_rows_of_grid(part):
    for axis, pairs, _ in ROUNDS:
        part = part + lax.ppermute(part, axis, pairs)
    return part


def sum_over_cols_of_grid(part):
    length = lax.axis_size(COLS)
    copies = jnp.broadcast_to(part[None], (length, *part.shape))
    return jnp.sum(lax.all_to_all(copies, COLS, 0, 0, tiled=True), axis=0)


def trade(pieces, pairing):
    out = [pieces[0]]
    for d in (1, 2, 3):
        out.append(lax.ppermute(pieces[d], ZC, flip(pairing, d // 2, d % 2)))
    return out


def body(covariance, factor_left, factor_right):
    start = 0
    traded = []
    for n in CHUNKS:
        groups = []
        for pairing in (1, 2):
            pieces = pack(covariance, factor_left if start == 0 else None, start, n)
            groups.append(trade(pieces, pairing))
            start += n
        traded.append(groups)

    got = []
    for groups in traded:
        whole = assemble(groups)
        got.append(lax.all_to_all(whole, SPREAD, 0, 0, tiled=True))

    panel = gather_right(factor_right)
    high, low = split(panel)
    right = jnp.concatenate([high, low, high, low])
    packed = got[0][:, TILE : TILE + 32, :].reshape(32, 32, 2, TILE)
    left = packed.transpose(0, 3, 2, 1).reshape(2048, 64)
    high, low = split(left)
    left = jnp.concatenate([high, high, low, low], axis=1)

    parts, row_parts, col_parts = [], [], []
    start = 0
    for i, n in enumerate(CHUNKS):
        first = TILE + 32 if i == 0 else TILE * n
        offsets = tuple(j * TILE for j in range(n)) + tuple(first + j * TILE for j in range(n))
        swapped = (False,) * n + (True,) * n
        part, row, col = correct(got[i], left, right[:, start * 128 : (start + 2 * n) * 128], 0, offsets, swapped)
        parts.append(part)
        row_parts.append(row[:, 0, :].reshape(16, 128))
        col_parts.append(jnp.sum(col, axis=0))
        start += 2 * n
    col_total = sum_over_rows_of_grid(jnp.concatenate(col_parts).reshape(8, 128)).reshape(1024)
    row_total = sum_over_cols_of_grid(sum(row_parts)).reshape(2048)
    row_factor = lax.rsqrt(jnp.sqrt(row_total / ORDER + epsilon))
    col_factor = lax.rsqrt(jnp.sqrt(col_total / ORDER + epsilon))
    return scale(parts, row_factor, col_factor)


def solution(mesh):
    fine = Mesh(mesh.devices.reshape(4, 2, 2, 2, 2, 2), NAMES)
    placed = (P(NAMES, None), P(None, NAMES), P(ROWS, COLS))
    return jax.shard_map(body, mesh=fine, in_specs=placed, out_specs=P(ROWS, COLS), check_vma=False)
```

```python
import functools

import jax
import jax.numpy as jnp
from jax import lax
from jax.experimental import pallas as pl
from jax.experimental.pallas import tpu as pltpu
from jax.sharding import Mesh
from jax.sharding import PartitionSpec as P


ORDER = 16384
TILE = 64
epsilon = 1e-06
F32 = jnp.float32

NAMES = ("y", "xl", "xh", "z1", "z0", "c")
ROWS = ("y", "xl")
COLS = ("xh", "z1", "z0", "c")
SPREAD = ("z0", "c", "xl", "xh", "z1")

CHUNKS = (3, 2, 2, 1)
WIDE = pltpu.CompilerParams(vmem_limit_bytes=56 * 1024 * 1024)
PARAMS = pltpu.CompilerParams(vmem_limit_bytes=24 * 1024 * 1024)


PARTS = 2
RUN = TILE // PARTS


def pack_kernel(count, with_left, *refs):
    out_ref = refs[count + with_left]
    low = lax.broadcasted_iota(jnp.int32, (RUN, 128), 1) < TILE
    for j in range(count):
        rows = slice(j * RUN, j * RUN + RUN)
        for m in range(8):
            xh, z1, z0 = m // 4, m // 2 % 2, m % 2
            a = refs[j][:, m * 128 : m * 128 + 128]
            b = refs[j][:, 1024 + m * 128 : 1024 + m * 128 + 128]
            out_ref[z0 * 2, 0, xh * 2 + z1, rows, :] = jnp.where(low, a, pltpu.roll(b, 64, 1))
            out_ref[z0 * 2 + 1, 0, xh * 2 + z1, rows, :] = jnp.where(low, pltpu.roll(a, 64, 1), b)
    if with_left:
        turned_ref = refs[-1]
        r, part = pl.program_id(0), pl.program_id(1)

        @pl.when((r == 0) & (part == 0))
        def _():
            left = refs[count][...]
            turned_ref[...] = jnp.transpose(jnp.concatenate([left, left], 0))

        half = RUN // 2
        at = pl.multiple_of(r * 64 + part * half, half)
        first = turned_ref[pl.ds(at, half), :]
        second = turned_ref[pl.ds(at + 32, half), :]
        packed = jnp.where(low[0:half], first, second)
        for to in range(4):
            for m in range(4):
                out_ref[to, 0, m, count * RUN : count * RUN + half, :] = packed


def pack(x, left, start, count):
    with_left = left is not None
    height = RUN * count + RUN // 2 * with_left
    in_specs = [pl.BlockSpec((RUN, 2048), lambda r, i, s=start + j: (r * PARTS + i, s)) for j in range(count)]
    args = [x] * count
    scratch = []
    if with_left:
        in_specs.append(pl.BlockSpec((64, 128), lambda r, i: (0, 0)))
        args.append(left)
        scratch.append(pltpu.VMEM((128, 128), F32))
    return pl.pallas_call(
        functools.partial(pack_kernel, count, with_left),
        grid=(2, PARTS),
        in_specs=in_specs,
        out_specs=pl.BlockSpec((4, 1, 4, height, 128), lambda r, i: (0, r, 0, i, 0)),
        out_shape=jax.ShapeDtypeStruct((4, 2, 4, height * PARTS, 128), F32),
        scratch_shapes=scratch,
        compiler_params=WIDE,
        name="pack",
    )(*args)


def deal_kernel(y_ref, *refs):
    for d in range(3):
        refs[3 + d][...] = refs[d][0]


def deal(got, y):
    height = got.shape[2]

    def spec(d):
        return pl.BlockSpec((1, 2, height, 128), lambda i, y: (y[0] ^ d, i, 0, 0))

    return pl.pallas_call(
        deal_kernel,
        grid_spec=pltpu.PrefetchScalarGridSpec(
            num_scalar_prefetch=1,
            grid=(4,),
            in_specs=[spec(d) for d in (1, 2, 3)],
            out_specs=[pl.BlockSpec((2, height, 128), lambda i, y: (i, 0, 0))] * 3,
        ),
        out_shape=[jax.ShapeDtypeStruct((8, height, 128), F32)] * 3,
        compiler_params=PARAMS,
        name="deal",
    )(y, got, got, got)


def piece_specs(height):
    return [pl.BlockSpec((1, 2, height, 128), lambda i, y: (y[0], i, 0, 0))] + [
        pl.BlockSpec((2, height, 128), lambda i, y: (i, 0, 0))
    ] * 3


def left_kernel(y_ref, own_ref, *refs):
    out_ref = refs[3]
    low = lax.broadcasted_iota(jnp.int32, (32, 128), 1) < TILE
    step = own_ref.shape[2] // PARTS
    for d in range(4):
        for k in range(2):
            rows = [slice(p * step + step - RUN // 2, p * step + step) for p in range(PARTS)]
            packed = jnp.concatenate([own_ref[0, k, r, :] if d == 0 else refs[d - 1][k, r, :] for r in rows], 0)
            other = pltpu.roll(packed, 64, 1)
            twice = jnp.concatenate([jnp.where(low, packed, other), jnp.where(low, other, packed)], 0)
            high = twice.astype(jnp.bfloat16)
            rest = (twice - high.astype(F32)).astype(jnp.bfloat16)
            to = slice(k * TILE, k * TILE + TILE)
            out_ref[y_ref[0] ^ d, 0, to, 0:128] = high
            out_ref[y_ref[0] ^ d, 0, to, 128:256] = rest


def left_factor(got, pieces, y):
    return pl.pallas_call(
        left_kernel,
        grid_spec=pltpu.PrefetchScalarGridSpec(
            num_scalar_prefetch=1,
            grid=(4,),
            in_specs=piece_specs(got.shape[2]),
            out_specs=pl.BlockSpec((4, 1, 128, 256), lambda i, y: (0, i, 0, 0)),
        ),
        out_shape=jax.ShapeDtypeStruct((4, 4, 128, 256), jnp.bfloat16),
        compiler_params=PARAMS,
        name="left",
    )(y, got, *pieces)


def correct_kernel(lanes, step, y_ref, own_ref, one_ref, two_ref, three_ref, left_ref, right_ref, out_ref, row_ref, col_ref):
    @pl.when(pl.program_id(0) == 0)
    def _():
        col_ref[...] = jnp.zeros_like(col_ref)

    col_acc = [jnp.zeros((8, 128), F32)] * lanes
    for d in range(4):
        home = y_ref[0] ^ d
        product = jnp.dot(left_ref[home, 0], right_ref[...], preferred_element_type=F32)
        row_acc = jnp.zeros((128, 128), F32)
        for j in range(lanes):
            cols = slice(j * 128, j * 128 + 128)
            tiles = []
            for k in range(2):
                for p in range(PARTS):
                    rows = slice(p * step + j * RUN, p * step + j * RUN + RUN)
                    tiles.append(own_ref[0, k, rows, :] if d == 0 else (one_ref, two_ref, three_ref)[d - 1][k, rows, :])
            tile = jnp.concatenate(tiles, 0) + product[:, cols]
            out_ref[home, 0, :, cols] = tile
            square = tile * tile
            row_acc = row_acc + square
            col_acc[j] = col_acc[j] + jnp.sum(square.reshape(16, 8, 128), 0)
        row_ref[home, 0] = jnp.sum(jnp.transpose(row_acc).reshape(16, 8, 128), 0)
    for j in range(lanes):
        col_ref[:, j * 128 : j * 128 + 128] += col_acc[j]


def correct(got, pieces, y, left, right, lanes):
    width = 128 * lanes
    height = got.shape[2]
    part, row, col = pl.pallas_call(
        functools.partial(correct_kernel, lanes, height // PARTS),
        grid_spec=pltpu.PrefetchScalarGridSpec(
            num_scalar_prefetch=1,
            grid=(4,),
            in_specs=piece_specs(height)
            + [
                pl.BlockSpec((4, 1, 128, 256), lambda i, y: (0, i, 0, 0)),
                pl.BlockSpec((256, width), lambda i, y: (0, 0)),
            ],
            out_specs=[
                pl.BlockSpec((4, 1, 128, width), lambda i, y: (0, i, 0, 0)),
                pl.BlockSpec((4, 1, 8, 128), lambda i, y: (0, i, 0, 0)),
                pl.BlockSpec((8, width), lambda i, y: (0, 0)),
            ],
        ),
        out_shape=[
            jax.ShapeDtypeStruct((4, 4, 128, width), F32),
            jax.ShapeDtypeStruct((4, 4, 8, 128), F32),
            jax.ShapeDtypeStruct((8, width), F32),
        ],
        compiler_params=PARAMS,
        name="correct",
    )(y, got, *pieces, left, right)
    return part.reshape(2048, width), row, col


def scale_kernel(widths, *refs):
    n = len(widths)
    row_ref, col_ref, out_ref = refs[n:]
    row = jnp.transpose(jnp.broadcast_to(row_ref[0], (128, 256)))
    at = 0
    for ref, width in zip(refs, widths):
        for j in range(width // 128):
            cols = slice(at, at + 128)
            out_ref[:, cols] = ref[:, j * 128 : j * 128 + 128] * (row * col_ref[:, cols])
            at += 128


def scale(parts, row, col):
    widths = tuple(p.shape[1] for p in parts)
    return pl.pallas_call(
        functools.partial(scale_kernel, widths),
        grid=(8,),
        in_specs=[pl.BlockSpec((256, w), lambda i: (i, 0)) for w in widths]
        + [pl.BlockSpec((1, 1, 256), lambda i: (i, 0, 0)), pl.BlockSpec((1, 1024), lambda i: (0, 0))],
        out_specs=pl.BlockSpec((256, 1024), lambda i: (i, 0)),
        out_shape=jax.ShapeDtypeStruct((2048, 1024), F32),
        compiler_params=PARAMS,
        name="scale",
    )(*parts, row.reshape(8, 1, 256), col.reshape(1, 1024))


def split(x):
    high = lax.reduce_precision(x, 8, 7)
    low = lax.reduce_precision(x - high, 8, 7)
    return high.astype(jnp.bfloat16), low.astype(jnp.bfloat16)


def flip(d):
    return [(i, i ^ d) for i in range(4)]


def gather_right(part):
    other = lax.ppermute(part, "xl", [(0, 1), (1, 0)])
    first = lax.axis_index("xl") == 0
    part = jnp.where(first, jnp.concatenate([part, other]), jnp.concatenate([other, part]))
    others = [part] + [lax.ppermute(part, "y", flip(d)) for d in (1, 2, 3)]
    y = lax.axis_index("y")
    for bit in (1, 2):
        first = (y & bit) == 0
        others = [jnp.where(first, others[d], others[d ^ bit]) for d in range(4)]
    return jnp.concatenate(others)


def sum_by_permutes(part, moves):
    for axis, d in moves:
        n = lax.axis_size(axis)
        part = part + lax.ppermute(part, axis, [(i, i ^ d) for i in range(n)])
    return part


def body(covariance, factor_left, factor_right):
    y = lax.axis_index("y").reshape(1).astype(jnp.int32)
    got, hops = [], []
    start = 0
    for i, n in enumerate(CHUNKS):
        whole = pack(covariance, factor_left if i == 0 else None, start, n)
        height = whole.shape[3]
        out = lax.all_to_all(whole.reshape(32, height, 128), SPREAD, 0, 0, tiled=True)
        got.append(out.reshape(4, 8, height, 128))
        pieces = deal(got[i], y)
        hops.append([lax.ppermute(p, "y", flip(d)) for p, d in zip(pieces, (1, 2, 3))])
        start += n

    panel = gather_right(factor_right)
    high, low = split(panel)
    right = jnp.concatenate([high, low, high, low])
    left = left_factor(got[0], hops[0], y)

    parts, row_parts, col_parts = [], [], []
    start = 0
    for i, n in enumerate(CHUNKS):
        part, row, col = correct(got[i], hops[i], y, left, right[:, start * 128 : (start + n) * 128], n)
        parts.append(part)
        row_parts.append(row)
        col_parts.append(col)
        start += n
    row_part = jnp.sum(sum(row_parts), axis=2).reshape(16, 128)
    col_part = jnp.sum(jnp.concatenate(col_parts, axis=1), axis=0).reshape(8, 128)
    row_total = sum_by_permutes(row_part, (("c", 1), ("z0", 1), ("z1", 1), ("xh", 1))).reshape(2048)
    col_total = sum_by_permutes(col_part, (("xl", 1), ("y", 1), ("y", 2))).reshape(1024)
    row_factor = lax.rsqrt(jnp.sqrt(row_total / ORDER + epsilon))
    col_factor = lax.rsqrt(jnp.sqrt(col_total / ORDER + epsilon))
    return scale(parts, row_factor, col_factor)


def solution(mesh):
    fine = Mesh(mesh.devices.reshape(4, 2, 2, 2, 2, 2), NAMES)
    placed = (P(NAMES, None), P(None, NAMES), P(ROWS, COLS))
    return jax.shard_map(body, mesh=fine, in_specs=placed, out_specs=P(ROWS, COLS), check_vma=False)
```

```python
import functools

import jax
import jax.numpy as jnp
from jax import lax
from jax.experimental import pallas as pl
from jax.experimental.pallas import tpu as pltpu
from jax.sharding import Mesh
from jax.sharding import PartitionSpec as P


ORDER = 16384
TILE = 64
epsilon = 1e-06
F32 = jnp.float32

NAMES = ("y", "xl", "xh", "z1", "z0", "c")
ROWS = ("y", "xl")
COLS = ("xh", "z1", "z0", "c")
SPREAD = ("z0", "c", "xl", "xh", "z1")

CHUNKS = (3, 2, 2, 1)
WIDE = pltpu.CompilerParams(vmem_limit_bytes=56 * 1024 * 1024)
PARAMS = pltpu.CompilerParams(vmem_limit_bytes=24 * 1024 * 1024)


PARTS = 1
RUN = TILE // PARTS


def pack_kernel(count, with_left, *refs):
    out_ref = refs[count + with_left]
    low = lax.broadcasted_iota(jnp.int32, (RUN, 128), 1) < TILE
    for j in range(count):
        rows = slice(j * RUN, j * RUN + RUN)
        for m in range(8):
            xh, z1, z0 = m // 4, m // 2 % 2, m % 2
            a = refs[j][:, m * 128 : m * 128 + 128]
            b = refs[j][:, 1024 + m * 128 : 1024 + m * 128 + 128]
            out_ref[z0 * 2, 0, xh * 2 + z1, rows, :] = jnp.where(low, a, pltpu.roll(b, 64, 1))
            out_ref[z0 * 2 + 1, 0, xh * 2 + z1, rows, :] = jnp.where(low, pltpu.roll(a, 64, 1), b)
    if with_left:
        turned_ref = refs[-1]
        r, part = pl.program_id(0), pl.program_id(1)

        @pl.when((r == 0) & (part == 0))
        def _():
            left = refs[count][...]
            turned_ref[...] = jnp.transpose(jnp.concatenate([left, left], 0))

        half = RUN // 2
        at = pl.multiple_of(r * 64 + part * half, half)
        first = turned_ref[pl.ds(at, half), :]
        second = turned_ref[pl.ds(at + 32, half), :]
        packed = jnp.where(low[0:half], first, second)
        for to in range(4):
            for m in range(4):
                out_ref[to, 0, m, count * RUN : count * RUN + half, :] = packed


def pack(x, left, start, count):
    with_left = left is not None
    height = RUN * count + RUN // 2 * with_left
    in_specs = [pl.BlockSpec((RUN, 2048), lambda r, i, s=start + j: (r * PARTS + i, s)) for j in range(count)]
    args = [x] * count
    scratch = []
    if with_left:
        in_specs.append(pl.BlockSpec((64, 128), lambda r, i: (0, 0)))
        args.append(left)
        scratch.append(pltpu.VMEM((128, 128), F32))
    return pl.pallas_call(
        functools.partial(pack_kernel, count, with_left),
        grid=(2, PARTS),
        in_specs=in_specs,
        out_specs=pl.BlockSpec((4, 1, 4, height, 128), lambda r, i: (0, r, 0, i, 0)),
        out_shape=jax.ShapeDtypeStruct((4, 2, 4, height * PARTS, 128), F32),
        scratch_shapes=scratch,
        compiler_params=WIDE,
        name="pack",
    )(*args)


def left_kernel(got_ref, out_ref):
    low = lax.broadcasted_iota(jnp.int32, (32, 128), 1) < TILE
    step = got_ref.shape[2] // PARTS
    for to in range(4):
        for k in range(2):
            rows = [slice(p * step + step - RUN // 2, p * step + step) for p in range(PARTS)]
            packed = jnp.concatenate([got_ref[to, k, r, :] for r in rows], 0)
            other = pltpu.roll(packed, 64, 1)
            twice = jnp.concatenate([jnp.where(low, packed, other), jnp.where(low, other, packed)], 0)
            high = twice.astype(jnp.bfloat16)
            rest = (twice - high.astype(F32)).astype(jnp.bfloat16)
            rows = slice(k * TILE, k * TILE + TILE)
            out_ref[to, 0, rows, 0:128] = high
            out_ref[to, 0, rows, 128:256] = rest


def left_factor(got):
    return pl.pallas_call(
        left_kernel,
        grid=(4,),
        in_specs=[pl.BlockSpec((4, 2, got.shape[2], 128), lambda i: (0, i, 0, 0))],
        out_specs=pl.BlockSpec((4, 1, 128, 256), lambda i: (0, i, 0, 0)),
        out_shape=jax.ShapeDtypeStruct((4, 4, 128, 256), jnp.bfloat16),
        compiler_params=PARAMS,
        name="left",
    )(got)


def correct_kernel(lanes, got_ref, left_ref, right_ref, *refs):
    row_ref, col_ref = refs[4:]
    step = got_ref.shape[2] // PARTS
    y = lax.axis_index("y")

    @pl.when(pl.program_id(0) == 0)
    def _():
        col_ref[...] = jnp.zeros_like(col_ref)

    col_acc = [jnp.zeros((8, 128), F32)] * lanes
    for d in range(4):
        to = y ^ d
        product = jnp.dot(left_ref[to, 0], right_ref[...], preferred_element_type=F32)
        row_acc = jnp.zeros((128, 128), F32)
        for j in range(lanes):
            cols = slice(j * 128, j * 128 + 128)
            tiles = []
            for k in range(2):
                for p in range(PARTS):
                    tiles.append(got_ref[to, k, p * step + j * RUN : p * step + j * RUN + RUN, :])
            tile = jnp.concatenate(tiles, 0) + product[:, cols]
            refs[d][:, cols] = tile
            square = tile * tile
            row_acc = row_acc + square
            col_acc[j] = col_acc[j] + jnp.sum(square.reshape(16, 8, 128), 0)
        row_ref[d, 0] = jnp.sum(jnp.transpose(row_acc).reshape(16, 8, 128), 0)
    for j in range(lanes):
        col_ref[:, j * 128 : j * 128 + 128] += col_acc[j]


def correct(got, left, right, lanes):
    width = 128 * lanes
    *pieces, row, col = pl.pallas_call(
        functools.partial(correct_kernel, lanes),
        grid=(4,),
        in_specs=[
            pl.BlockSpec((4, 2, got.shape[2], 128), lambda i: (0, i, 0, 0)),
            pl.BlockSpec((4, 1, 128, 256), lambda i: (0, i, 0, 0)),
            pl.BlockSpec((256, width), lambda i: (0, 0)),
        ],
        out_specs=[pl.BlockSpec((128, width), lambda i: (i, 0))] * 4
        + [
            pl.BlockSpec((4, 1, 8, 128), lambda i: (0, i, 0, 0)),
            pl.BlockSpec((8, width), lambda i: (0, 0)),
        ],
        out_shape=[jax.ShapeDtypeStruct((512, width), F32)] * 4
        + [
            jax.ShapeDtypeStruct((4, 4, 8, 128), F32),
            jax.ShapeDtypeStruct((8, width), F32),
        ],
        compiler_params=PARAMS,
        name="correct",
    )(got, left, right)
    return pieces, row, col


def scale_kernel(widths, *refs):
    n = len(widths)
    row_ref, col_ref, out_ref = refs[4 * n :]
    y = lax.axis_index("y")
    for d in range(4):
        row = jnp.transpose(jnp.broadcast_to(row_ref[d, 0], (128, 128)))
        at = 0
        for i, width in enumerate(widths):
            for j in range(width // 128):
                cols = slice(at, at + 128)
                out_ref[y ^ d, 0, :, cols] = refs[4 * i + d][:, j * 128 : j * 128 + 128] * (row * col_ref[:, cols])
                at += 128


def scale(chunks, row, col):
    widths = tuple(pieces[0].shape[1] for pieces in chunks)
    out = pl.pallas_call(
        functools.partial(scale_kernel, widths),
        grid=(4,),
        in_specs=[pl.BlockSpec((128, w), lambda i: (i, 0)) for w in widths for _ in range(4)]
        + [pl.BlockSpec((4, 1, 1, 128), lambda i: (0, i, 0, 0)), pl.BlockSpec((1, 1024), lambda i: (0, 0))],
        out_specs=pl.BlockSpec((4, 1, 128, 1024), lambda i: (0, i, 0, 0)),
        out_shape=jax.ShapeDtypeStruct((4, 4, 128, 1024), F32),
        compiler_params=PARAMS,
        name="scale",
    )(*[p for pieces in chunks for p in pieces], row.reshape(4, 4, 1, 128), col.reshape(1, 1024))
    return out.reshape(2048, 1024)


def split(x):
    high = lax.reduce_precision(x, 8, 7)
    low = lax.reduce_precision(x - high, 8, 7)
    return high.astype(jnp.bfloat16), low.astype(jnp.bfloat16)


def flip(d):
    return [(i, i ^ d) for i in range(4)]


def gather_right(part):
    other = lax.ppermute(part, "xl", [(0, 1), (1, 0)])
    first = lax.axis_index("xl") == 0
    part = jnp.where(first, jnp.concatenate([part, other]), jnp.concatenate([other, part]))
    others = [part] + [lax.ppermute(part, "y", flip(d)) for d in (1, 2, 3)]
    y = lax.axis_index("y")
    for bit in (1, 2):
        first = (y & bit) == 0
        others = [jnp.where(first, others[d], others[d ^ bit]) for d in range(4)]
    return jnp.concatenate(others)


def sum_over(part, axes):
    n = lax.axis_size(axes)
    total = part
    for d in range(1, n):
        total = total + lax.ppermute(part, axes, [(i, i ^ d) for i in range(n)])
    return total


def body(covariance, factor_left, factor_right):
    panel = gather_right(factor_right)
    high, low = split(panel)
    right = jnp.concatenate([high, low, high, low])

    chunks, row_parts, col_parts, held = [], [], [], []
    start = 0
    for i, n in enumerate(CHUNKS):
        whole = pack(covariance, factor_left if i == 0 else None, start, n)
        height = whole.shape[3]
        out = lax.all_to_all(whole.reshape(32, height, 128), SPREAD, 0, 0, tiled=True)
        got = out.reshape(4, 8, height, 128)
        if i == 0:
            left = left_factor(got)
        pieces, row, col = correct(got, left, right[:, start * 128 : (start + n) * 128], n)
        held.append(pieces)
        row_parts.append(row)
        col_parts.append(col)
        start += n
        if i == len(CHUNKS) - 2:
            row_early = lax.optimization_barrier(jnp.sum(sum(row_parts), axis=2))
    row_part = row_early + jnp.sum(row_parts[-1], axis=2)
    col_part = jnp.sum(jnp.concatenate(col_parts, axis=1), axis=0).reshape(8, 128)
    rows, col = [row_part[0]], col_part
    for d in (1, 2, 3):
        both = jnp.concatenate([row_part[d], col_part])
        both = lax.ppermute(both, "y", flip(d))
        rows.append(both[:4])
        col = col + both[4:]
    col_total = sum_over(col, "xl")
    row_total = jnp.stack(rows).reshape(16, 128)
    for axes in (("xh", "c"), ("z1", "z0")):
        row_total = sum_over(row_total, axes)
    row_factor = lax.rsqrt(jnp.sqrt(row_total / ORDER + epsilon))
    col_factor = lax.rsqrt(jnp.sqrt(col_total / ORDER + epsilon))
    for pieces in held:
        chunks.append([pieces[0]] + [lax.ppermute(pieces[d], "y", flip(d)) for d in (1, 2, 3)])
    return scale(chunks, row_factor, col_factor)


def solution(mesh):
    fine = Mesh(mesh.devices.reshape(4, 2, 2, 2, 2, 2), NAMES)
    placed = (P(NAMES, None), P(None, NAMES), P(ROWS, COLS))
    return jax.shard_map(body, mesh=fine, in_specs=placed, out_specs=P(ROWS, COLS), check_vma=False)
```

```python
import functools

import jax
import jax.numpy as jnp
from jax import lax
from jax.experimental import pallas as pl
from jax.experimental.pallas import tpu as pltpu
from jax.sharding import Mesh
from jax.sharding import PartitionSpec as P


ORDER = 16384
TILE = 64
epsilon = 1e-06
F32 = jnp.float32

NAMES = ("y", "xl", "xh", "z1", "z0", "c")
ROWS = ("y", "xl")
COLS = ("xh", "z1", "z0", "c")
SPREAD = ("z0", "c", "xl", "xh", "z1")

CHUNKS = (3, 2, 2, 1)
WIDE = pltpu.CompilerParams(vmem_limit_bytes=56 * 1024 * 1024)
PARAMS = pltpu.CompilerParams(vmem_limit_bytes=24 * 1024 * 1024)


PARTS = 1
RUN = TILE // PARTS


def pack_kernel(count, with_left, *refs):
    out_ref = refs[count + with_left]
    low = lax.broadcasted_iota(jnp.int32, (RUN, 128), 1) < TILE
    for j in range(count):
        rows = slice(j * RUN, j * RUN + RUN)
        for m in range(8):
            xh, z1, z0 = m // 4, m // 2 % 2, m % 2
            a = refs[j][:, m * 128 : m * 128 + 128]
            b = refs[j][:, 1024 + m * 128 : 1024 + m * 128 + 128]
            out_ref[z0 * 2, 0, xh * 2 + z1, rows, :] = jnp.where(low, a, pltpu.roll(b, 64, 1))
            out_ref[z0 * 2 + 1, 0, xh * 2 + z1, rows, :] = jnp.where(low, pltpu.roll(a, 64, 1), b)
    if with_left:
        turned_ref = refs[-1]
        r, part = pl.program_id(0), pl.program_id(1)

        @pl.when((r == 0) & (part == 0))
        def _():
            left = refs[count][...]
            turned_ref[...] = jnp.transpose(jnp.concatenate([left, left], 0))

        half = RUN // 2
        at = pl.multiple_of(r * 64 + part * half, half)
        first = turned_ref[pl.ds(at, half), :]
        second = turned_ref[pl.ds(at + 32, half), :]
        packed = jnp.where(low[0:half], first, second)
        for to in range(4):
            for m in range(4):
                out_ref[to, 0, m, count * RUN : count * RUN + half, :] = packed


def pack(x, left, start, count):
    with_left = left is not None
    height = RUN * count + RUN // 2 * with_left
    in_specs = [pl.BlockSpec((RUN, 2048), lambda r, i, s=start + j: (r * PARTS + i, s)) for j in range(count)]
    args = [x] * count
    scratch = []
    if with_left:
        in_specs.append(pl.BlockSpec((64, 128), lambda r, i: (0, 0)))
        args.append(left)
        scratch.append(pltpu.VMEM((128, 128), F32))
    return pl.pallas_call(
        functools.partial(pack_kernel, count, with_left),
        grid=(2, PARTS),
        in_specs=in_specs,
        out_specs=pl.BlockSpec((4, 1, 4, height, 128), lambda r, i: (0, r, 0, i, 0)),
        out_shape=jax.ShapeDtypeStruct((4, 2, 4, height * PARTS, 128), F32),
        scratch_shapes=scratch,
        compiler_params=WIDE,
        name="pack",
    )(*args)


def left_kernel(got_ref, out_ref):
    low = lax.broadcasted_iota(jnp.int32, (32, 128), 1) < TILE
    step = got_ref.shape[2] // PARTS
    for to in range(4):
        for k in range(2):
            rows = [slice(p * step + step - RUN // 2, p * step + step) for p in range(PARTS)]
            packed = jnp.concatenate([got_ref[to, k, r, :] for r in rows], 0)
            other = pltpu.roll(packed, 64, 1)
            twice = jnp.concatenate([jnp.where(low, packed, other), jnp.where(low, other, packed)], 0)
            high = twice.astype(jnp.bfloat16)
            rest = (twice - high.astype(F32)).astype(jnp.bfloat16)
            rows = slice(k * TILE, k * TILE + TILE)
            out_ref[to, 0, rows, 0:128] = high
            out_ref[to, 0, rows, 128:256] = rest


def left_factor(got):
    return pl.pallas_call(
        left_kernel,
        grid=(4,),
        in_specs=[pl.BlockSpec((4, 2, got.shape[2], 128), lambda i: (0, i, 0, 0))],
        out_specs=pl.BlockSpec((4, 1, 128, 256), lambda i: (0, i, 0, 0)),
        out_shape=jax.ShapeDtypeStruct((4, 4, 128, 256), jnp.bfloat16),
        compiler_params=PARAMS,
        name="left",
    )(got)


def correct_kernel(start, lanes, got_ref, left_ref, right_ref, *refs):
    row_ref, col_ref = refs[4:]
    step = got_ref.shape[2] // PARTS
    y = lax.axis_index("y")

    @pl.when(pl.program_id(0) == 0)
    def _():
        col_ref[...] = jnp.zeros_like(col_ref)

    right = right_ref[:, start * 128 : (start + lanes) * 128]
    col_acc = [jnp.zeros((8, 128), F32)] * lanes
    for d in range(4):
        to = y ^ d
        product = jnp.dot(left_ref[to, 0], right, preferred_element_type=F32)
        row_acc = jnp.zeros((128, 128), F32)
        for j in range(lanes):
            cols = slice(j * 128, j * 128 + 128)
            tiles = []
            for k in range(2):
                for p in range(PARTS):
                    tiles.append(got_ref[to, k, p * step + j * RUN : p * step + j * RUN + RUN, :])
            tile = jnp.concatenate(tiles, 0) + product[:, cols]
            refs[d][:, cols] = tile
            square = tile * tile
            row_acc = row_acc + square
            col_acc[j] = col_acc[j] + jnp.sum(square.reshape(16, 8, 128), 0)
        row_ref[d, 0] = jnp.sum(jnp.transpose(row_acc).reshape(16, 8, 128), 0)
    for j in range(lanes):
        col_ref[:, j * 128 : j * 128 + 128] += col_acc[j]


def correct(got, left, right, start, lanes):
    width = 128 * lanes
    *pieces, row, col = pl.pallas_call(
        functools.partial(correct_kernel, start, lanes),
        grid=(4,),
        in_specs=[
            pl.BlockSpec((4, 2, got.shape[2], 128), lambda i: (0, i, 0, 0)),
            pl.BlockSpec((4, 1, 128, 256), lambda i: (0, i, 0, 0)),
            pl.BlockSpec((256, 1024), lambda i: (0, 0)),
        ],
        out_specs=[pl.BlockSpec((128, width), lambda i: (i, 0))] * 4
        + [
            pl.BlockSpec((4, 1, 8, 128), lambda i: (0, i, 0, 0)),
            pl.BlockSpec((8, width), lambda i: (0, 0)),
        ],
        out_shape=[jax.ShapeDtypeStruct((512, width), F32)] * 4
        + [
            jax.ShapeDtypeStruct((4, 4, 8, 128), F32),
            jax.ShapeDtypeStruct((8, width), F32),
        ],
        compiler_params=PARAMS,
        name="correct",
    )(got, left, right)
    return pieces, row, col


def scale_kernel(widths, *refs):
    n = len(widths)
    row_ref, col_ref, out_ref = refs[4 * n :]
    y = lax.axis_index("y")
    for d in range(4):
        row = jnp.transpose(jnp.broadcast_to(row_ref[d, 0], (128, 128)))
        at = 0
        for i, width in enumerate(widths):
            for j in range(width // 128):
                cols = slice(at, at + 128)
                out_ref[y ^ d, 0, :, cols] = refs[4 * i + d][:, j * 128 : j * 128 + 128] * (row * col_ref[:, cols])
                at += 128


def scale(chunks, row, col):
    widths = tuple(pieces[0].shape[1] for pieces in chunks)
    out = pl.pallas_call(
        functools.partial(scale_kernel, widths),
        grid=(4,),
        in_specs=[pl.BlockSpec((128, w), lambda i: (i, 0)) for w in widths for _ in range(4)]
        + [pl.BlockSpec((4, 1, 1, 128), lambda i: (0, i, 0, 0)), pl.BlockSpec((1, 1024), lambda i: (0, 0))],
        out_specs=pl.BlockSpec((4, 1, 128, 1024), lambda i: (0, i, 0, 0)),
        out_shape=jax.ShapeDtypeStruct((4, 4, 128, 1024), F32),
        compiler_params=PARAMS,
        name="scale",
    )(*[p for pieces in chunks for p in pieces], row.reshape(4, 4, 1, 128), col.reshape(1, 1024))
    return out.reshape(2048, 1024)


def split(x):
    high = lax.reduce_precision(x, 8, 7)
    low = lax.reduce_precision(x - high, 8, 7)
    return high.astype(jnp.bfloat16), low.astype(jnp.bfloat16)


def flip(d):
    return [(i, i ^ d) for i in range(4)]


def gather_right(part):
    other = lax.ppermute(part, "xl", [(0, 1), (1, 0)])
    first = lax.axis_index("xl") == 0
    part = jnp.where(first, jnp.concatenate([part, other]), jnp.concatenate([other, part]))
    others = [part] + [lax.ppermute(part, "y", flip(d)) for d in (1, 2, 3)]
    y = lax.axis_index("y")
    for bit in (1, 2):
        first = (y & bit) == 0
        others = [jnp.where(first, others[d], others[d ^ bit]) for d in range(4)]
    return jnp.concatenate(others)


def sum_over(part, axes):
    n = lax.axis_size(axes)
    total = part
    for d in range(1, n):
        total = total + lax.ppermute(part, axes, [(i, i ^ d) for i in range(n)])
    return total


def body(covariance, factor_left, factor_right):
    panel = gather_right(factor_right)
    high, low = split(panel)
    right = jnp.concatenate([high, low, high, low])

    chunks, row_parts, col_parts, held = [], [], [], []
    start = 0
    for i, n in enumerate(CHUNKS):
        whole = pack(covariance, factor_left if i == 0 else None, start, n)
        height = whole.shape[3]
        out = lax.all_to_all(whole.reshape(32, height, 128), SPREAD, 0, 0, tiled=True)
        got = out.reshape(4, 8, height, 128)
        if i == 0:
            left = left_factor(got)
        pieces, row, col = correct(got, left, right, start, n)
        held.append(pieces)
        row_parts.append(row)
        col_parts.append(col)
        start += n
        if i == len(CHUNKS) - 2:
            row_early = lax.optimization_barrier(jnp.sum(sum(row_parts), axis=2))
    row_part = row_early + jnp.sum(row_parts[-1], axis=2)
    col_part = jnp.sum(jnp.concatenate(col_parts, axis=1), axis=0).reshape(8, 128)
    rows, col = [row_part[0]], col_part
    for d in (1, 2, 3):
        both = jnp.concatenate([row_part[d], col_part])
        both = lax.ppermute(both, "y", flip(d))
        rows.append(both[:4])
        col = col + both[4:]
    col_total = sum_over(col, "xl")
    row_total = jnp.stack(rows).reshape(16, 128)
    for axes in (("xh", "c"), ("z1", "z0")):
        row_total = sum_over(row_total, axes)
    row_factor = lax.rsqrt(jnp.sqrt(row_total / ORDER + epsilon))
    col_factor = lax.rsqrt(jnp.sqrt(col_total / ORDER + epsilon))
    for pieces in held:
        chunks.append([pieces[0]] + [lax.ppermute(pieces[d], "y", flip(d)) for d in (1, 2, 3)])
    return scale(chunks, row_factor, col_factor)


def solution(mesh):
    fine = Mesh(mesh.devices.reshape(4, 2, 2, 2, 2, 2), NAMES)
    placed = (P(NAMES, None), P(None, NAMES), P(ROWS, COLS))
    return jax.shard_map(body, mesh=fine, in_specs=placed, out_specs=P(ROWS, COLS), check_vma=False)
```
